1024 devices in a mesh: section: 2 (over core), group: 8 (over y), expert: 64 (over x, z).
Axes of the slice: x: 4, y: 8, z: 16, core: 2. Of those that a mesh axis runs over, the one named last changes fastest.
Arguments:
- tokens: bfloat16 [16, 4096, 2048], P('group', 'expert'), parts along dimension 0
- chosen: int32 [2, 16, 8, 64], P('section', 'group'), parts along dimension 1, may hold values from 0 to 4095, as said below
- norm_gain: float32 [2, 2048], P('section'), may hold values from 0.25 to 1.75
- router: bfloat16 [2, 2048, 8], P('section'), may hold values from -0.25 to 0.25
- w_in: bfloat16 [2, 64, 2048, 1024], P('section', 'expert'), may hold values from -0.125 to 0.125
- w_out: bfloat16 [2, 64, 1024, 2048], P('section', 'expert'), may hold values from -0.0625 to 0.0625
Outputs:
- outputs: bfloat16 [2, 16, 4096, 2048], P('section', 'group', 'expert'), parts along dimension 1
The draws below stay inside these ranges and needn't reach their ends.
There are 8 independent parts, one for each index of `group`. The reference program is written for one: setup_inputs(seed, part) draws one part's arguments, and reference() takes and returns one part's arrays. A program takes and returns all parts, laid end to end along the dimension named above; an argument that names none is the same for every part. Nothing has to cross between parts.
Inputs may be any that keep to these rules, and one draw needn't show every extreme that they name: `chosen`: for each section, micro-batch and expert the 64 indices are distinct and in no particular order. Of one device's tokens (an aligned block of 64 indices) an expert chooses at most 2; in every draw some expert chooses exactly 2 from some block.
All inputs are finite; a program needn't handle non-finite values.
Results may differ from the reference program's by a relative error of at most 0.001.
Values may be sent and summed in bfloat16 or wider, within the bound.
No kernel may reach another device: no remote copies, remote signals or barrier semaphores. Data moves between devices by JAX's collectives and lax.ppermute only.
A program may use at most 64 MiB of HBM per device.

```python
import math
import jax
import jax.numpy as jnp
from jax import lax

D = 2048
FF = 8192
TOK_DEV = 64
MICRO = 2
SLOT = 2
EXPERTS = 8
SPLIT = 8
TOK_MB = 4096
CAP = 64
N_SECTION = 2
N_EXPERT = 64


def draw_tokens(key, part):
    key_base, key_rows, key_cols = jax.random.split(key, 3)
    shape = (MICRO, TOK_MB, D)
    base = jax.random.normal(key_base, shape, jnp.float32)
    row_scale = jnp.exp(jax.random.uniform(key_rows, (MICRO, TOK_MB, 1), jnp.float32, math.log(0.3), math.log(3.0)))
    col_scale = jnp.exp(jax.random.uniform(key_cols, (D,), jnp.float32, -math.log(2.0), math.log(2.0)))
    return (base * row_scale * col_scale).astype(jnp.bfloat16)


def chosen_list(key):
    key_order, key_shift, key_score, key_shuffle = jax.random.split(key, 4)
    half_slot = SLOT // 2
    order = jax.random.permutation(key_order, N_EXPERT)
    shifts = jax.random.randint(key_shift, (N_EXPERT // 2,), -half_slot, half_slot + 1)
    shifts = shifts.at[0].set(half_slot)
    paired = jnp.stack([half_slot + shifts, half_slot - shifts], axis=1).reshape(N_EXPERT)
    counts = jnp.zeros((N_EXPERT,), jnp.int32).at[order].set(paired.astype(jnp.int32))
    scores = jax.random.randint(key_score, (N_EXPERT, TOK_DEV), 0, 1 << 20) * 1024 + jnp.arange(TOK_DEV, dtype=jnp.int32)[None, :]
    ranks = jnp.argsort(jnp.argsort(scores, axis=1, stable=True), axis=1, stable=True)
    picked = ranks < counts[:, None]
    positions = jnp.nonzero(picked.reshape(-1), size=CAP)[0].astype(jnp.int32)
    shuffle = jax.random.permutation(key_shuffle, CAP)
    return positions[shuffle].astype(jnp.int32)


def draw_chosen(key, part):
    keys = jax.random.split(jax.random.fold_in(key, 7), N_SECTION * MICRO * EXPERTS)
    lists = jax.vmap(chosen_list)(keys)
    return lists.reshape(N_SECTION, MICRO, EXPERTS, CAP).astype(jnp.int32)


def block_scale(key, dims, cuts, smallest, high):
    def one(dim, shards_of):
        heights = jax.random.uniform(jax.random.fold_in(jax.random.fold_in(key, 6), dim), (shards_of,), jnp.float32, smallest / len(cuts), high / len(cuts))
        return jnp.repeat(jnp.exp(heights), dims[dim] // shards_of).reshape((-1,) + (1,) * (len(dims) - dim - 1))

    gain = one(*cuts[0])
    for cut in cuts[1:]:
        gain = gain * one(*cut)
    return gain


def scatter_about(key, extent, spread, bound, shards=(), kind=jnp.bfloat16):
    level = block_scale(key, extent, shards, -0.22, 0.18) if shards else 1.0
    values = jax.random.normal(key, extent, jnp.float32) * spread * level
    return jnp.minimum(jnp.maximum(values, -bound), bound).astype(kind)


def setup_inputs(seed: int = 0, part: int = 0) -> dict:
    splits = jax.random.split(jax.random.key(seed), 7)
    part_splits = jax.random.split(jax.random.fold_in(splits[6], part), 7)
    tokens = draw_tokens(jax.random.fold_in(jax.random.fold_in(splits[6], part), 71), part)
    chosen = draw_chosen(jax.random.fold_in(jax.random.fold_in(splits[6], part), 71), part)
    norm_gain = jnp.clip(1.0 + 0.15 * jax.random.normal(splits[2], (N_SECTION, D), jnp.float32), 0.25, 1.75)
    router = scatter_about(splits[3], (N_SECTION, D, EXPERTS), (D // 4) ** -0.5, 0.25, ((0, 2),))
    w_in = scatter_about(splits[4], (N_SECTION, N_EXPERT, D, FF // SPLIT), D ** -0.5, 0.125, ((0, 2), (1, 64)))
    w_out = scatter_about(splits[5], (N_SECTION, N_EXPERT, FF // SPLIT, D), FF ** -0.5, 0.0625, ((0, 2), (1, 64)))
    return {"tokens": tokens, "chosen": chosen, "norm_gain": norm_gain, "router": router, "w_in": w_in, "w_out": w_out}


def expert_layer(act, gain_row, router_cols, w_first, w_second, chosen_now):
    floats = act.astype(jnp.float32)
    inverse_rms = lax.rsqrt(lax.optimization_barrier(jnp.mean(floats * floats, axis=-1, keepdims=True)) + 1e-06)
    normed = (floats * inverse_rms * gain_row).astype(jnp.bfloat16)
    gate_all = jax.nn.sigmoid(jnp.dot(normed, router_cols, preferred_element_type=jnp.float32))
    hidden_each = FF // SPLIT
    w_first_all = w_first.reshape(EXPERTS, SPLIT, D, hidden_each).transpose(0, 2, 1, 3).reshape(EXPERTS, D, FF)
    w_second_all = w_second.reshape(EXPERTS, FF, D)

    def one_expert(items):
        first_mat, second_mat, token_ids, column = items
        picked = normed[token_ids]
        hidden = jax.nn.gelu(jnp.dot(picked, first_mat, preferred_element_type=jnp.float32), approximate=True).astype(jnp.bfloat16)
        result = jnp.dot(hidden, second_mat, preferred_element_type=jnp.float32)
        weights = gate_all[token_ids, column]
        return result * weights[:, None]
    results = lax.map(one_expert, (w_first_all, w_second_all, chosen_now, jnp.arange(EXPERTS, dtype=jnp.int32)))
    combined = jnp.zeros((TOK_MB, D), jnp.float32).at[chosen_now.reshape(-1)].add(results.reshape(-1, D))
    return (floats + combined).astype(jnp.bfloat16)

def reference(tokens, chosen, norm_gain, router, w_in, w_out):
    section_rows = []
    previous = [tokens[batch_at] for batch_at in range(MICRO)]
    for section_at in range(N_SECTION):
        current = []
        for batch_at in range(MICRO):
            layer_out = expert_layer(previous[batch_at], norm_gain[section_at], router[section_at], w_in[section_at], w_out[section_at], chosen[section_at, batch_at])
            current.append(layer_out)
        section_rows.append(jnp.stack(current))
        previous = current
    return jnp.stack(section_rows)
```

```python
import jax
import jax.numpy as jnp
from jax import lax
from jax.sharding import PartitionSpec as P

SWAP = [(0, 1), (1, 0)]


def layer(current, picks, gain_row, router_cols, own, other, use_own, device, owners, shards_each):
    tok_rows, width = current.shape
    experts, capacity = picks.shape
    slots = 2 * capacity // owners
    floats = current.astype(jnp.float32)
    inverse_rms = lax.rsqrt(jnp.mean(floats * floats, axis=-1, keepdims=True) + 1e-06)
    normed = (floats * inverse_rms * gain_row).astype(jnp.bfloat16)
    gate_all = jax.nn.sigmoid(jnp.dot(normed, router_cols, preferred_element_type=jnp.float32))
    local_idx = picks - device * tok_rows
    tok_hit = local_idx[:, :, None] == jnp.arange(tok_rows, dtype=jnp.int32)[None, None, :]
    chosen_here = tok_hit.any(axis=1).astype(jnp.int32)
    rank = jnp.cumsum(chosen_here, axis=1) - 1
    selector = (
        (rank[:, None, :] == jnp.arange(slots, dtype=jnp.int32)[None, :, None])
        & (chosen_here[:, None, :] > 0)
    ).astype(jnp.float32)
    flat_select = selector.reshape(experts * slots, tok_rows)
    gate_slot = jnp.einsum("xst,tx->xs", selector, gate_all, precision=lax.Precision.HIGHEST)
    dispatched = jnp.dot(
        flat_select.astype(jnp.bfloat16), normed, preferred_element_type=jnp.float32
    ).astype(jnp.bfloat16)
    outgoing = jnp.broadcast_to(
        dispatched.reshape(experts, 1, slots, width), (experts, shards_each, slots, width)
    ).reshape(owners, slots, width)
    arrived = lax.all_to_all(outgoing, "expert", split_axis=0, concat_axis=0, tiled=True)

    def ffn(rows, first, second):
        hidden = jax.nn.gelu(
            jnp.dot(rows, first, preferred_element_type=jnp.float32), approximate=True
        ).astype(jnp.bfloat16)
        return jnp.dot(hidden, second, preferred_element_type=jnp.float32).astype(jnp.bfloat16)

    rows = arrived.reshape(-1, width)
    partial_value = lax.cond(
        use_own,
        lambda r, a, b: ffn(r, *a),
        lambda r, a, b: ffn(r, *b),
        rows,
        own,
        other,
    ).reshape(owners, slots, width)
    returned = lax.all_to_all(partial_value, "expert", split_axis=0, concat_axis=0, tiled=True)
    summed = (
        returned.reshape(experts, shards_each, slots, width).astype(jnp.float32).sum(axis=1)
    )
    weighted = summed * gate_slot[:, :, None]
    contrib = jnp.dot(
        flat_select.T, weighted.reshape(experts * slots, width), precision=lax.Precision.HIGHEST
    )
    return (floats + contrib).astype(jnp.bfloat16)


def local(tokens, chosen, norm_gain, router, w_in, w_out):
    owners = lax.axis_size("expert")
    core = lax.axis_index("section")
    device = lax.axis_index("expert")
    experts = chosen.shape[2]
    shards_each = owners // experts

    def swap(value):
        return lax.ppermute(value, "section", SWAP)

    first = core == 0
    own = (w_in[0, 0], w_out[0, 0])
    other = (swap(own[0]), swap(own[1]))
    small_other = (swap(chosen[0]), swap(norm_gain[0]), swap(router[0]))
    small_own = (chosen[0], norm_gain[0], router[0])
    current = lax.dynamic_index_in_dim(tokens, core, 0, keepdims=False)
    results = []
    for section in range(2):
        use_own = core == section
        picks, gain_row, router_cols = (
            jnp.where(use_own, a, b) for a, b in zip(small_own, small_other)
        )
        picks = lax.dynamic_index_in_dim(picks, core, 0, keepdims=False)
        current = layer(
            current, picks, gain_row, router_cols, own, other, use_own, device, owners, shards_each
        )
        results.append(current)
    got = swap(jnp.where(first, results[1], results[0]))
    return jnp.where(
        first, jnp.stack([results[0], got]), jnp.stack([got, results[1]])
    )[None]


def solution(mesh):
    placed = (
        P("group", "expert", None),
        P("section", "group", None, None),
        P("section", None),
        P("section", None, None),
        P("section", "expert", None, None),
        P("section", "expert", None, None),
    )
    return jax.shard_map(
        local,
        mesh=mesh,
        in_specs=placed,
        out_specs=P("section", "group", "expert", None),
        check_vma=False,
    )
```

```python
import jax
import jax.numpy as jnp
from jax import lax
from jax.experimental import pallas as pl
from jax.experimental.pallas import tpu as pltpu
from jax.sharding import PartitionSpec as P

SWAP = [(0, 1), (1, 0)]
STAGGER_NS = 14000


def hold_kernel(core_ref, value_ref, out_ref):
    @pl.when(core_ref[0] == 1)
    def _():
        pl.delay(STAGGER_NS)

    out_ref[...] = value_ref[...]


def hold(value, core):
    return pl.pallas_call(
        hold_kernel,
        out_shape=jax.ShapeDtypeStruct(value.shape, value.dtype),
        in_specs=[
            pl.BlockSpec(memory_space=pltpu.SMEM),
            pl.BlockSpec(memory_space=pltpu.VMEM),
        ],
        out_specs=pl.BlockSpec(memory_space=pltpu.VMEM),
    )(core.reshape(1), value)


def layer(current, picks, gain_row, router_cols, own, other, use_own, device, owners, shards_each):
    tok_rows, width = current.shape
    experts, capacity = picks.shape
    slots = 2 * capacity // owners
    floats = current.astype(jnp.float32)
    inverse_rms = lax.rsqrt(jnp.mean(floats * floats, axis=-1, keepdims=True) + 1e-06)
    normed = (floats * inverse_rms * gain_row).astype(jnp.bfloat16)
    gate_all = jax.nn.sigmoid(jnp.dot(normed, router_cols, preferred_element_type=jnp.float32))
    local_idx = picks - device * tok_rows
    tok_hit = local_idx[:, :, None] == jnp.arange(tok_rows, dtype=jnp.int32)[None, None, :]
    chosen_here = tok_hit.any(axis=1).astype(jnp.int32)
    rank = jnp.cumsum(chosen_here, axis=1) - 1
    selector = (
        (rank[:, None, :] == jnp.arange(slots, dtype=jnp.int32)[None, :, None])
        & (chosen_here[:, None, :] > 0)
    ).astype(jnp.float32)
    flat_select = selector.reshape(experts * slots, tok_rows)
    gate_slot = jnp.einsum("xst,tx->xs", selector, gate_all, precision=lax.Precision.HIGHEST)
    dispatched = jnp.dot(
        flat_select.astype(jnp.bfloat16), normed, preferred_element_type=jnp.float32
    ).astype(jnp.bfloat16)
    outgoing = jnp.broadcast_to(
        dispatched.reshape(experts, 1, slots, width), (experts, shards_each, slots, width)
    ).reshape(owners, slots, width)
    arrived = lax.all_to_all(outgoing, "expert", split_axis=0, concat_axis=0, tiled=True)


    def ffn(rows, first, second):
        hidden = jax.nn.gelu(
            jnp.dot(rows, first, preferred_element_type=jnp.float32), approximate=True
        ).astype(jnp.bfloat16)
        return jnp.dot(hidden, second, preferred_element_type=jnp.float32).astype(jnp.bfloat16)

    partial_value = lax.cond(
        use_own,
        lambda r, a, b: ffn(r, *a),
        lambda r, a, b: ffn(r, *b),
        arrived.reshape(-1, width),
        own,
        other,
    ).reshape(owners, slots, width)
    returned = lax.all_to_all(partial_value, "expert", split_axis=0, concat_axis=0, tiled=True)
    summed = (
        returned.reshape(experts, shards_each, slots, width).astype(jnp.float32).sum(axis=1)
    )
    weighted = summed * gate_slot[:, :, None]
    contrib = jnp.dot(
        flat_select.T, weighted.reshape(experts * slots, width), precision=lax.Precision.HIGHEST
    )
    return (floats + contrib).astype(jnp.bfloat16)


def local(tokens, chosen, norm_gain, router, w_in, w_out):
    owners = lax.axis_size("expert")
    core = lax.axis_index("section")
    device = lax.axis_index("expert")
    experts = chosen.shape[2]
    shards_each = owners // experts

    def swap(value):
        return lax.ppermute(value, "section", SWAP)

    first = core == 0
    micro, capacity = chosen.shape[1], chosen.shape[3]
    width = tokens.shape[2]
    packed = jnp.concatenate(
        [
            norm_gain,
            router[0].astype(jnp.float32).T,
            jnp.pad(chosen[0].astype(jnp.float32).reshape(1, -1), ((0, 0), (0, -chosen.size % width))),
        ]
    )
    packed_other = swap(packed)
    own = (w_in[0, 0], w_out[0, 0])
    other = (swap(own[0]), swap(own[1]))
    current = lax.dynamic_index_in_dim(tokens, core, 0, keepdims=False)
    results = []
    for section in range(2):
        use_own = core == section
        small = jnp.where(use_own, packed, packed_other)
        gain_row = small[:1]
        router_cols = small[1 : 1 + experts].astype(jnp.bfloat16).T
        picks = small[1 + experts, : chosen.size].astype(jnp.int32).reshape(micro, experts, capacity)
        picks = lax.dynamic_index_in_dim(picks, core, 0, keepdims=False)
        if section == 0:
            picks = hold(picks, core)
        current = layer(
            current,
            picks,
            gain_row,
            router_cols,
            own,
            other,
            use_own,
            device,
            owners,
            shards_each,
        )
        results.append(current)
    got = swap(jnp.where(first, results[1], results[0]))
    return jnp.where(
        first, jnp.stack([results[0], got]), jnp.stack([got, results[1]])
    )[None]


def solution(mesh):
    placed = (
        P("group", "expert", None),
        P("section", "group", None, None),
        P("section", None),
        P("section", None, None),
        P("section", "expert", None, None),
        P("section", "expert", None, None),
    )
    return jax.shard_map(
        local,
        mesh=mesh,
        in_specs=placed,
        out_specs=P("section", "group", "expert", None),
        check_vma=False,
    )
```
